32 devices in a mesh: dp: 2 (over x), tp: 16 (over z, y, core).
Axes of the slice: x: 2, y: 2, z: 4, core: 2. Of those that a mesh axis runs over, the one named last changes fastest.
Arguments:
- hidden: bfloat16 [128, 9, 2048], P('dp'), parts along dimension 0
- norm_gain: float32 [2048], replicated
- w_head: bfloat16 [2048, 128256], P(None, 'tp')
- draft_probs: float32 [128, 8, 128256], P('dp', None, 'tp'), parts along dimension 0
- draft_tokens: int32 [128, 8], P('dp'), parts along dimension 0
- temperature: float32 [128], P('dp'), parts along dimension 0
Outputs:
- output 1: float32 [128, 8], P('dp'), parts along dimension 0
- output 2: float32 [128, 8], P('dp'), parts along dimension 0
- output 3: float32 [128, 8, 128256], P('dp', None, 'tp'), parts along dimension 0
- output 4: float32 [128], P('dp'), parts along dimension 0
There are 2 independent parts. The reference program is written for one: setup_inputs(seed, part) draws one part's arguments, and reference() takes and returns one part's arrays. A program takes and returns all parts, laid end to end along the dimension named above; an argument that names none is the same for every part.
All inputs are finite; a program needn't handle non-finite values.
Results may differ from the reference program's by a relative error of at most 0.001.
Values sent between devices are 32-bit elements.
A program may use at most 1 GiB of HBM per device.

```python
import jax
import jax.numpy as jnp
from jax import lax

BATCH_ROWS = 64
DRAFT_LEN = 8
D_MODEL = 2048
VOCAB_SIZE = 128256
CLUSTER_COUNT = 3
WEIGHT_BLOCK = 128
CLUSTER_SPAN = VOCAB_SIZE // 32


def setup_inputs(seed: int = 0, part: int = 0) -> dict:
    part_key = jax.random.fold_in(jax.random.key(seed), part)
    key_h, key_q, key_s, key_t, key_c, key_k, key_o = jax.random.split(part_key, 7)
    key_w, key_g = jax.random.split(jax.random.key(seed + 1), 2)
    hidden = jax.random.normal(key_h, (BATCH_ROWS, DRAFT_LEN + 1, D_MODEL), jnp.float32).astype(jnp.bfloat16)
    norm_gain = jax.random.uniform(key_g, (D_MODEL,), jnp.float32, 0.5, 1.5)

    def weight_block(block_idx):
        gauss_block = jax.random.normal(jax.random.fold_in(key_w, block_idx), (WEIGHT_BLOCK, VOCAB_SIZE), jnp.float32)
        return (gauss_block * D_MODEL ** -0.5).astype(jnp.bfloat16)

    w_head = lax.map(weight_block, jnp.arange(D_MODEL // WEIGHT_BLOCK)).reshape(D_MODEL, VOCAB_SIZE)
    q_scale = jax.random.uniform(key_s, (BATCH_ROWS, DRAFT_LEN, 1), jnp.float32, 0.7, 1.3)
    q_logits = jax.random.normal(key_q, (BATCH_ROWS, DRAFT_LEN, VOCAB_SIZE), jnp.float32) * q_scale
    draft_probs = jax.nn.softmax(q_logits, axis=-1)
    temperature = jax.random.uniform(key_t, (BATCH_ROWS,), jnp.float32, 0.6, 1.4)
    centers = jax.random.randint(key_c, (CLUSTER_COUNT,), 0, VOCAB_SIZE - CLUSTER_SPAN)
    choice = jax.random.randint(key_k, (BATCH_ROWS, DRAFT_LEN), 0, CLUSTER_COUNT)
    offsets = jax.random.randint(key_o, (BATCH_ROWS, DRAFT_LEN), 0, CLUSTER_SPAN)
    draft_tokens = (centers[choice] + offsets).astype(jnp.int32)
    return {'hidden': hidden, 'norm_gain': norm_gain, 'w_head': w_head, 'draft_probs': draft_probs, 'draft_tokens': draft_tokens, 'temperature': temperature}


def reference(hidden, norm_gain, w_head, draft_probs, draft_tokens, temperature):
    def one_row(row_args):
        row_hidden, row_probs, row_tokens, row_temp = row_args
        hidden_f32 = row_hidden.astype(jnp.float32)
        inv_rms = lax.rsqrt(jnp.mean(hidden_f32 * hidden_f32, axis=-1, keepdims=True) + 1e-5)
        normed = (hidden_f32 * inv_rms * norm_gain).astype(jnp.bfloat16)
        logits = jnp.dot(normed, w_head, preferred_element_type=jnp.float32)
        scaled = logits / row_temp
        row_max = jnp.max(scaled, axis=-1, keepdims=True)
        row_lse = row_max + jnp.log(jnp.sum(jnp.exp(scaled - row_max), axis=-1, keepdims=True))
        target = jnp.exp(scaled[:DRAFT_LEN] - row_lse[:DRAFT_LEN])
        tok_target = jnp.take_along_axis(target, row_tokens[:, None], axis=-1)[:, 0]
        tok_draft = jnp.take_along_axis(row_probs, row_tokens[:, None], axis=-1)[:, 0]
        accept = jnp.minimum(1.0, tok_target / tok_draft)
        excess = jnp.maximum(target - row_probs, 0.0)
        norm_sum = jnp.sum(excess, axis=-1)
        residual = excess / norm_sum[:, None]
        return accept, norm_sum, residual, row_lse[DRAFT_LEN, 0]

    accept, norm_sum, residual, bonus_lse = lax.map(one_row, (hidden, draft_probs, draft_tokens, temperature))
    return accept, norm_sum, residual, bonus_lse
```

```python
import functools
import math

import jax
import jax.numpy as jnp
from jax import lax
from jax.experimental import pallas as pl
from jax.experimental.pallas import tpu as pltpu
from jax.sharding import PartitionSpec as P

F32 = jnp.float32
BF16 = jnp.bfloat16
LOG2E = math.log2(math.e)
LN2 = math.log(2.0)
TILE = 512
SLOTS = 4
MESH = pl.DeviceIdType.MESH


def _main_kernel(n_dev, n_seq, draft, d_model, vocab,
                 g_ref, dt_ref, t_ref, h_hbm, w_hbm, q_hbm,
                 ex_ref, inv_ref, st_ref,
                 h_scr, x_ref, wbuf, q_scr, za, zb, c_ref, rel_ref, m_ref, s_ref,
                 az_ref, aq_ref, mt_ref, send1, send2, send3, recv1, recv2, recv3,
                 hsem, wsem, qsem, ssem1, ssem2, ssem3, rsem1, rsem2, rsem3):
    rows = n_seq * draft
    n_all = rows + n_seq
    n_tiles = pl.cdiv(vocab, TILE)
    last_w = vocab - (n_tiles - 1) * TILE
    last_k = pl.cdiv(last_w, 128)
    last_lanes = last_w - (last_k - 1) * 128
    n_blk = rows // 128
    me = lax.axis_index("tp")
    peers = [lax.rem(me + k, n_dev) for k in range(1, n_dev)]

    barrier = pltpu.get_barrier_semaphore()
    for p in peers:
        pl.semaphore_signal(barrier, inc=1, device_id={"tp": p}, device_id_type=MESH)

    def h_copy(j):
        return pltpu.make_async_copy(h_hbm.at[j], h_scr.at[j], hsem.at[j])

    def w_copy(t, width=TILE):
        slot = lax.rem(t, SLOTS) if not isinstance(t, int) else t % SLOTS
        start = t * TILE
        return pltpu.make_async_copy(
            w_hbm.at[pl.ds(start, width), :], wbuf.at[slot, pl.ds(0, width), :], wsem.at[slot])

    def q_copy(t, width=TILE):
        cols = pl.ds(t * TILE, width) if isinstance(t, int) else pl.ds(pl.multiple_of(t * TILE, TILE), width)
        return pltpu.make_async_copy(q_hbm.at[:, cols], q_scr.at[:, cols], qsem.at[t])

    def tile_copies(t):
        width = last_w if isinstance(t, int) and t == n_tiles - 1 else TILE
        return w_copy(t, width), q_copy(t, width)

    for j in range(draft + 1):
        h_copy(j).start()
    for t in range(3):
        for cp in tile_copies(t):
            cp.start()

    lane8 = lax.broadcasted_iota(jnp.int32, (8, 128), 1)

    t_row = t_ref[...]
    d_f = dt_ref[...].astype(F32)
    base = me * vocab
    lane_s = lax.broadcasted_iota(jnp.int32, (draft, n_seq), 1)
    t_all = jnp.broadcast_to(LOG2E / t_row, (draft, n_seq))
    for b in range(n_seq):
        pick = lane_s == b
        r8 = slice(b * draft, (b + 1) * draft)
        c = jnp.sum(jnp.where(pick, t_all, 0.0), axis=1, keepdims=True)
        d = jnp.sum(jnp.where(pick, d_f, 0.0), axis=1, keepdims=True)
        c_ref[r8, :] = jnp.broadcast_to(c, (draft, 128))
        loc = jnp.broadcast_to(d, (draft, 128)).astype(jnp.int32) - base
        owned = (loc >= 0) & (loc < vocab)
        rel_ref[r8, :] = jnp.where(owned, loc - lane8, -vocab)
    diag = lax.broadcasted_iota(jnp.int32, (n_seq, n_seq), 0) == lax.broadcasted_iota(jnp.int32, (n_seq, n_seq), 1)
    cb = jnp.sum(jnp.where(diag, jnp.broadcast_to(LOG2E / t_row, (n_seq, n_seq)), 0.0), axis=1, keepdims=True)
    c_ref[rows:n_all, :] = jnp.broadcast_to(cb, (n_seq, 128))

    m_ref[...] = jnp.full(m_ref.shape, -jnp.inf, F32)
    s_ref[...] = jnp.zeros(s_ref.shape, F32)
    m_ref[n_all:, :] = jnp.zeros((m_ref.shape[0] - n_all, 128), F32)
    s_ref[n_all:, :] = jnp.ones((m_ref.shape[0] - n_all, 128), F32)
    az_ref[...] = jnp.full(az_ref.shape, -jnp.inf, F32)
    aq_ref[...] = jnp.full(aq_ref.shape, -1.0, F32)

    n_lane = d_model // 128
    for j in range(draft + 1):
        h_copy(j).wait()
        acc = None
        for k in range(n_lane):
            hv = h_scr[j, :, k * 128:(k + 1) * 128].astype(F32)
            acc = hv * hv if acc is None else acc + hv * hv
        r = lax.rsqrt(jnp.sum(acc, axis=1, keepdims=True) * (1.0 / d_model) + 1e-5)
        r = jnp.broadcast_to(r, (n_seq, 128))
        for k in range(n_lane):
            cols = slice(k * 128, (k + 1) * 128)
            xv = h_scr[j, :, cols].astype(F32) * r * g_ref[:, cols]
            if j < draft:
                mt_ref[k, j * n_seq:(j + 1) * n_seq, :] = xv
            else:
                x_ref[rows:n_all, cols] = xv.astype(BF16)
    for b in range(0, n_seq, 2):
        for k in range(n_lane):
            cols = slice(k * 128, (k + 1) * 128)
            lo = mt_ref[k, pl.ds(b, draft, stride=n_seq), :]
            hi = mt_ref[k, pl.ds(b + 1, draft, stride=n_seq), :]
            x_ref[b * draft:(b + 2) * draft, cols] = jnp.concatenate([lo, hi], axis=0).astype(BF16)

    def dot(t, zref, kn=TILE // 128):
        slot = lax.rem(t, SLOTS) if not isinstance(t, int) else t % SLOTS
        w = wbuf[slot, 0:kn * 128, :]
        zref[:, 0:kn * 128] = lax.dot_general(
            x_ref[...], w, (((1,), (1,)), ((), ())), preferred_element_type=F32)

    def epilogue(t, zref, kn=TILE // 128, last=False):
        start = t * TILE
        for r in range(n_all // 8):
            rs = slice(r * 8, r * 8 + 8)
            zs = [zref[rs, k * 128:(k + 1) * 128] for k in range(kn)]
            if last:
                zs[-1] = jnp.where(lane8 < last_lanes, zs[-1], -jnp.inf)
            c = c_ref[rs, :]
            zm = functools.reduce(jnp.maximum, zs)
            m2 = zm * c
            es = [jnp.exp2(z * c - m2) for z in zs]
            st = functools.reduce(jnp.add, es)
            mo = m_ref[rs, :]
            mn = jnp.maximum(mo, m2)
            s_ref[rs, :] = s_ref[rs, :] * jnp.exp2(mo - mn) + st * jnp.exp2(m2 - mn)
            m_ref[rs, :] = mn
            if r * 8 >= rows:
                continue
            mt_ref[t, rs, :] = m2
            rel = rel_ref[rs, :]
            az, aq = az_ref[rs, :], aq_ref[rs, :]
            for k in range(kn):
                wd = 128 if not (last and k == kn - 1) else last_lanes
                if isinstance(t, int):
                    cs = pl.ds(start + k * 128, wd)
                else:
                    cs = pl.ds(pl.multiple_of(start + k * 128, 128), wd)
                if wd == 128:
                    ex_ref[rs, cs] = es[k]
                    qv = q_scr[rs, cs]
                    hit = rel == start + k * 128
                    az = jnp.where(hit, zs[k], az)
                    aq = jnp.where(hit, qv, aq)
                else:
                    ex_ref[rs, cs] = es[k][:, :wd]
                    qv = jnp.concatenate([q_scr[rs, cs], jnp.zeros((8, 128 - wd), F32)], axis=1)
                    hit = rel == start + k * 128
                    az = jnp.where(hit, zs[k], az)
                    aq = jnp.where(hit, qv, aq)
            az_ref[rs, :] = az
            aq_ref[rs, :] = aq

    w_copy(0).wait()
    dot(0, za)

    def pair(i, carry):
        t1 = 2 * i + 1
        t2 = 2 * i + 2

        @pl.when(i < (n_tiles - 2) // 2 - 1)
        def _():
            for cp in tile_copies(t1 + 2) + tile_copies(t2 + 2):
                cp.start()

        @pl.when(i == (n_tiles - 2) // 2 - 1)
        def _():
            for cp in tile_copies(n_tiles - 1):
                cp.start()

        w_copy(t1).wait()
        q_copy(t1 - 1).wait()
        w_copy(t2).wait()
        q_copy(t1).wait()
        dot(t1, zb)
        epilogue(t1 - 1, za)
        dot(t2, za)
        epilogue(t1, zb)
        return carry

    lax.fori_loop(0, (n_tiles - 2) // 2, pair, 0)
    w_copy(n_tiles - 1, last_w).wait()
    q_copy(n_tiles - 2).wait()
    q_copy(n_tiles - 1, last_w).wait()
    dot(n_tiles - 1, zb, last_k)
    epilogue(n_tiles - 2, za)
    epilogue(n_tiles - 1, zb, last_k, True)

    def exchange(src, dst, ssem, rsem):
        out = []
        for k, p in enumerate(peers):
            cp = pltpu.make_async_remote_copy(
                src_ref=src, dst_ref=dst.at[me], send_sem=ssem.at[k], recv_sem=rsem.at[me],
                device_id={"tp": p}, device_id_type=MESH)
            cp.start()
            out.append(cp)
        return out

    def finish(cps, src, dst, rsem):
        for p in peers:
            pltpu.make_async_remote_copy(
                src_ref=src, dst_ref=dst.at[p], send_sem=rsem.at[p], recv_sem=rsem.at[p],
                device_id={"tp": p}, device_id_type=MESH).wait_recv()

    def drain(cps):
        for cp in cps:
            cp.wait_send()

    def spread(row):
        return jnp.transpose(jnp.broadcast_to(row, (128, 128)))

    for i in range(n_blk + 1):
        blk = slice(i * 128, (i + 1) * 128)
        mt = jnp.transpose(m_ref[blk, :])
        st = jnp.transpose(s_ref[blk, :])
        mrow = jnp.max(mt, axis=0, keepdims=True)
        srow = jnp.sum(st * jnp.exp2(mt - mrow), axis=0, keepdims=True)
        send1[i:i + 1, :] = mrow + jnp.log(srow) * LOG2E
    send1[n_blk + 1:, :] = jnp.zeros((8 - n_blk - 1, 128), F32)
    send2[...] = jnp.zeros((8, 128), F32)
    send3[...] = jnp.zeros((8, 128), F32)

    pl.semaphore_wait(barrier, n_dev - 1)
    cps1 = exchange(send1, recv1, ssem1, rsem1)
    recv1[me] = send1[...]

    s_tok, q_tok = [], []
    for i in range(n_blk):
        blk = slice(i * 128, (i + 1) * 128)
        s_tok.append(jnp.max(jnp.transpose(az_ref[blk, :] * c_ref[blk, :]), axis=0, keepdims=True))
        q_tok.append(jnp.max(jnp.transpose(aq_ref[blk, :]), axis=0, keepdims=True))
    s_tok = jnp.concatenate(s_tok, axis=0)
    q_tok = jnp.concatenate(q_tok, axis=0)

    finish(cps1, send1, recv1, rsem1)
    parts = [recv1[i] for i in range(n_dev)]
    mx = functools.reduce(jnp.maximum, parts)
    tot = functools.reduce(jnp.add, [jnp.exp2(v - mx) for v in parts])
    lse2 = mx + jnp.log(tot) * LOG2E

    acc_loc = jnp.where(q_tok >= 0.0, jnp.minimum(1.0, jnp.exp2(s_tok - lse2[0:n_blk]) / q_tok), 0.0)
    send2[0:n_blk, :] = acc_loc
    cps2 = exchange(send2, recv2, ssem2, rsem2)
    recv2[me] = send2[...]

    for i in range(n_blk):
        m_ref[i * 128:(i + 1) * 128, :] = spread(lse2[i:i + 1, :])

    n_full = vocab // 128
    tail = vocab - n_full * 128

    def excess(r, carry):
        rs = pl.ds(pl.multiple_of(r * 8, 8), 8)
        lb = m_ref[rs, :]
        accs = [jnp.zeros((8, 128), F32) for _ in range(4)]
        for t in range(n_tiles):
            coef = jnp.exp2(mt_ref[t, rs, :] - lb)
            for k in range(TILE // 128):
                v = t * (TILE // 128) + k
                if v < n_full:
                    cs = slice(v * 128, (v + 1) * 128)
                    d = jnp.maximum(ex_ref[rs, cs] * coef - q_scr[rs, cs], 0.0)
                    ex_ref[rs, cs] = d
                    accs[k] = accs[k] + d
                elif v == n_full and tail:
                    cs = slice(v * 128, v * 128 + tail)
                    d = jnp.maximum(ex_ref[rs, cs] * coef[:, :tail] - q_scr[rs, cs], 0.0)
                    ex_ref[rs, cs] = d
                    accs[k] = accs[k] + jnp.concatenate([d, jnp.zeros((8, 128 - tail), F32)], axis=1)
        s_ref[rs, :] = (accs[0] + accs[1]) + (accs[2] + accs[3])
        return carry

    lax.fori_loop(0, rows // 8, excess, 0)
    for i in range(n_blk):
        blk = slice(i * 128, (i + 1) * 128)
        send3[i:i + 1, :] = jnp.sum(jnp.transpose(s_ref[blk, :]), axis=0, keepdims=True)
    cps3 = exchange(send3, recv3, ssem3, rsem3)
    recv3[me] = send3[...]

    finish(cps2, send2, recv2, rsem2)
    acc_all = functools.reduce(jnp.add, [recv2[i] for i in range(n_dev)])
    st_ref[16:17, :] = lse2[n_blk:n_blk + 1, :] * LN2

    def by_seq(dense, scr):
        for i in range(n_blk):
            scr[i * 128:(i + 1) * 128, :] = spread(dense[i:i + 1, :])
        out = jnp.zeros((8, 128), F32)
        for b in range(n_seq):
            out = jnp.where(lane8 == b, scr[b * draft:(b + 1) * draft, :], out)
        return out

    st_ref[0:8, :] = by_seq(acc_all, az_ref)
    finish(cps3, send3, recv3, rsem3)
    norm = functools.reduce(jnp.add, [recv3[i] for i in range(n_dev)])
    st_ref[8:16, :] = by_seq(norm, aq_ref)
    inv = 1.0 / norm[0:n_blk, :]
    for i in range(n_blk):
        inv_ref[i * 128:(i + 1) * 128, :] = spread(inv[i:i + 1, :])
    drain(cps1)
    drain(cps2)
    drain(cps3)


def _scale_kernel(n_seq, draft, vocab, ex_ref, inv_ref, st_ref,
                  acc_ref, norm_ref, res_hbm, lse_ref, buf, sem):
    rows = n_seq * draft
    step = buf.shape[1]
    n = rows // step
    slots = buf.shape[0]

    def copy(i):
        slot = lax.rem(i, slots) if not isinstance(i, int) else i % slots
        return pltpu.make_async_copy(
            buf.at[slot], res_hbm.at[pl.ds(pl.multiple_of(i * step, step), step), :], sem.at[slot])

    n_full = vocab // 128
    tail = vocab - n_full * 128

    def body(i, carry):
        slot = lax.rem(i, slots)

        @pl.when(i >= slots)
        def _():
            copy(i - slots).wait()

        for r in range(step // 8):
            rs = pl.ds(pl.multiple_of(i * step + r * 8, 8), 8)
            inv = inv_ref[rs, :]
            for v in range(n_full):
                cs = slice(v * 128, (v + 1) * 128)
                buf[slot, r * 8:r * 8 + 8, cs] = ex_ref[rs, cs] * inv
            if tail:
                cs = slice(n_full * 128, vocab)
                buf[slot, r * 8:r * 8 + 8, cs] = ex_ref[rs, cs] * inv[:, :tail]
        copy(i).start()
        return carry

    lax.fori_loop(0, n, body, 0)
    acc_ref[...] = st_ref[0:draft, 0:n_seq]
    norm_ref[...] = st_ref[8:8 + draft, 0:n_seq]
    lse_ref[...] = st_ref[16:17, 0:n_seq]
    for s in range(slots):
        copy(n - slots + s).wait()


def solution(mesh):
    n_dev = mesh.shape["tp"]

    def local_step(hidden, norm_gain, w_head, draft_probs, draft_tokens, value_a11):
        n_seq, n_pos, d_model = hidden.shape
        draft = n_pos - 1
        vocab = w_head.shape[1]
        rows = n_seq * draft
        n_all = rows + n_seq
        n_tiles = pl.cdiv(vocab, TILE)
        h = jnp.transpose(hidden, (1, 0, 2))
        w = jnp.transpose(w_head)
        q = draft_probs.reshape(rows, vocab)
        vm = pl.BlockSpec(memory_space=pltpu.VMEM)
        anyspec = pl.BlockSpec(memory_space=pl.ANY)
        dma = pltpu.SemaphoreType.DMA
        stat = pltpu.VMEM((n_all + 64, 128), F32)
        ex, inv, st = pl.pallas_call(
            functools.partial(_main_kernel, n_dev, n_seq, draft, d_model, vocab),
            out_shape=(
                pltpu.VMEM((rows, vocab), F32),
                pltpu.VMEM((rows, 128), F32),
                pltpu.VMEM((24, 128), F32),
            ),
            in_specs=[vm, vm, vm, anyspec, anyspec, anyspec],
            out_specs=(vm, vm, vm),
            scratch_shapes=[
                pltpu.VMEM((n_pos, n_seq, d_model), BF16),
                pltpu.VMEM((n_all, d_model), BF16),
                pltpu.VMEM((SLOTS, TILE, d_model), BF16),
                pltpu.VMEM((rows, vocab), F32),
                pltpu.VMEM((n_all, TILE), F32),
                pltpu.VMEM((n_all, TILE), F32),
                pltpu.VMEM((n_all, 128), F32),
                pltpu.VMEM((rows, 128), jnp.int32),
                stat, stat,
                pltpu.VMEM((rows, 128), F32),
                pltpu.VMEM((rows, 128), F32),
                pltpu.VMEM((n_tiles, rows, 128), F32),
                pltpu.VMEM((8, 128), F32),
                pltpu.VMEM((8, 128), F32),
                pltpu.VMEM((8, 128), F32),
                pltpu.VMEM((n_dev, 8, 128), F32),
                pltpu.VMEM((n_dev, 8, 128), F32),
                pltpu.VMEM((n_dev, 8, 128), F32),
                dma((n_pos,)), dma((SLOTS,)), dma((n_tiles,)),
                dma((n_dev,)), dma((n_dev,)), dma((n_dev,)),
                dma((n_dev,)), dma((n_dev,)), dma((n_dev,)),
            ],
            compiler_params=pltpu.CompilerParams(
                collective_id=0, has_side_effects=True, vmem_limit_bytes=46 * 2**20),
        )(norm_gain.reshape(1, d_model), jnp.transpose(draft_tokens), value_a11.reshape(1, n_seq), h, w, q)

        vmc = lambda a: pltpu.with_memory_space_constraint(a, pltpu.VMEM)
        acc, norm, res, lse = pl.pallas_call(
            functools.partial(_scale_kernel, n_seq, draft, vocab),
            out_shape=(
                jax.ShapeDtypeStruct((draft, n_seq), F32),
                jax.ShapeDtypeStruct((draft, n_seq), F32),
                jax.ShapeDtypeStruct((rows, vocab), F32),
                jax.ShapeDtypeStruct((1, n_seq), F32),
            ),
            in_specs=[vm, vm, vm],
            out_specs=(vm, vm, anyspec, vm),
            scratch_shapes=[pltpu.VMEM((8, 16, vocab), F32), dma((8,))],
            compiler_params=pltpu.CompilerParams(vmem_limit_bytes=16 * 2**20),
        )(vmc(ex), vmc(inv), vmc(st))
        return (jnp.transpose(acc), jnp.transpose(norm), res.reshape(n_seq, draft, vocab), lse.reshape(n_seq))

    return jax.shard_map(
        local_step,
        mesh=mesh,
        in_specs=(P('dp', None, None), P(), P(None, 'tp'), P('dp', None, 'tp'), P('dp', None), P('dp')),
        out_specs=(P('dp', None), P('dp', None), P('dp', None, 'tp'), P('dp')),
        check_vma=False,
    )
```

```python
import functools
import math

import jax
import jax.numpy as jnp
from jax import lax
from jax.experimental import pallas as pl
from jax.experimental.pallas import tpu as pltpu
from jax.sharding import PartitionSpec as P

F32 = jnp.float32
BF16 = jnp.bfloat16
LOG2E = math.log2(math.e)
LN2 = math.log(2.0)
TILE = 512
SLOTS = 9
BODY = 4
UNROLL = 4
HALVED = 5
CHUNK = 32
MESH = pl.DeviceIdType.MESH


def _main_kernel(n_dev, n_seq, draft, d_model, vocab,
                 g_hbm, dt_hbm, t_hbm, h_hbm, w_hbm, q_hbm,
                 ex_ref, st_ref,
                 g_ref, dt_ref, t_ref, x_ref, wbuf, q_scr, za, zb, c_ref, rel_ref, m_ref, s_ref,
                 az_ref, aq_ref, mt_ref, send1, send2, send3, send4, recv1, recv2, recv3, recv4,
                 isem, hsem, wsem, qsem, ssem1, ssem2, ssem3, ssem4, rsem1, rsem2, rsem3, rsem4):
    rows = n_seq * draft
    n_all = rows + n_seq
    n_tiles = pl.cdiv(vocab, TILE)
    last_w = vocab - (n_tiles - 1) * TILE
    last_k = pl.cdiv(last_w, 128)
    last_lanes = last_w - (last_k - 1) * 128
    n_blk = rows // 128
    n_full = vocab // 128
    tail = vocab - n_full * 128
    stride = n_seq + 1
    me = lax.axis_index("tp")
    peers = [lax.rem(me + k, n_dev) for k in range(1, n_dev)]

    def h_dst(j):
        if j < draft:
            return wbuf.at[SLOTS - 1, pl.ds(j * n_seq, n_seq), :]
        return wbuf.at[SLOTS - 2, pl.ds(0, n_seq), :]

    def h_val(j, b0, nb, cols):
        if j < draft:
            return wbuf[SLOTS - 1, j * n_seq + b0:j * n_seq + b0 + nb, cols].astype(F32)
        return wbuf[SLOTS - 2, b0:b0 + nb, cols].astype(F32)

    def h_copy(j):
        return pltpu.make_async_copy(h_hbm.at[j], h_dst(j), hsem.at[j])

    def w_copy(t):
        if isinstance(t, int):
            slot, width = t % SLOTS, (last_w if t == n_tiles - 1 else TILE)
        else:
            slot, width = lax.rem(t, SLOTS), TILE
        return pltpu.make_async_copy(
            w_hbm.at[pl.ds(t * TILE, width), :], wbuf.at[slot, pl.ds(0, width), :], wsem.at[slot])

    def q_copy(t):
        if isinstance(t, int):
            cols = pl.ds(t * TILE, last_w if t == n_tiles - 1 else TILE)
        else:
            cols = pl.ds(pl.multiple_of(t * TILE, TILE), TILE)
        return pltpu.make_async_copy(q_hbm.at[:, cols], q_scr.at[:, cols], qsem.at[t])

    small = [pltpu.make_async_copy(src, dst, isem.at[i]) for i, (src, dst) in enumerate(
        ((dt_hbm, dt_ref), (t_hbm, t_ref), (g_hbm, g_ref)))]
    small[2].start()
    for j in [draft] + list(range(draft)):
        h_copy(j).start()
    w_copy(0).start()
    small[0].start()
    small[1].start()

    barrier = pltpu.get_barrier_semaphore()
    for p in peers:
        pl.semaphore_signal(barrier, inc=1, device_id={"tp": p}, device_id_type=MESH)

    lane8 = lax.broadcasted_iota(jnp.int32, (8, 128), 1)
    m_ref[...] = jnp.full(m_ref.shape, -jnp.inf, F32)
    s_ref[...] = jnp.zeros(s_ref.shape, F32)
    az_ref[...] = jnp.full(az_ref.shape, -jnp.inf, F32)
    n_lane = d_model // 128

    half_seq = n_seq // 2

    def inv_rms(j, b0, nb):
        acc = None
        for k in range(n_lane):
            hv = h_val(j, b0, nb, slice(k * 128, (k + 1) * 128))
            acc = hv * hv if acc is None else acc + hv * hv
        r = lax.rsqrt(jnp.sum(acc, axis=1, keepdims=True) * (1.0 / d_model) + 1e-5)
        return jnp.broadcast_to(r, (nb, 128))

    def normed(j, b0, nb, r):
        for k in range(n_lane):
            cols = slice(k * 128, (k + 1) * 128)
            xv = h_val(j, b0, nb, cols) * r * g_ref[:, cols]
            if j < draft:
                mt_ref[k, j * stride + b0:j * stride + b0 + nb, :] = xv
            else:
                x_ref[0:n_seq, cols] = xv.astype(BF16)

    def reorder(b0, nb):
        for b in range(b0, b0 + nb, 2):
            for k in range(n_lane):
                cols = slice(k * 128, (k + 1) * 128)
                lo = mt_ref[k, pl.ds(b, draft, stride=stride), :]
                hi = mt_ref[k, pl.ds(b + 1, draft, stride=stride), :]
                x_ref[n_seq + b * draft:n_seq + (b + 2) * draft, cols] = jnp.concatenate([lo, hi], axis=0).astype(BF16)

    def norm_some(js, b0, nb, wait=False):
        for n, j in enumerate(js):
            if n == 0:
                if wait:
                    h_copy(j).wait()
                r = inv_rms(j, b0, nb[0])
            r_next = None
            if n + 1 < len(js):
                if wait and n % 4 == 0:
                    for ahead in js[n + 1:n + 5]:
                        h_copy(ahead).wait()
                r_next = inv_rms(js[n + 1], b0, nb[n + 1])
            normed(j, b0, nb[n], r)
            r = r_next
            if wait and n == 4:
                for t in range(1, SLOTS - 2):
                    w_copy(t).start()

    small[2].wait()
    norm_some([draft] + list(range(draft)), 0, [n_seq] + [half_seq] * draft, True)
    reorder(0, half_seq)

    def dot(t, zref, part):
        kn = last_k if isinstance(t, int) and t == n_tiles - 1 else TILE // 128
        slot = lax.rem(t, SLOTS) if not isinstance(t, int) else t % SLOTS
        zref[part, 0:kn * 128] = lax.dot_general(
            x_ref[part, :], wbuf[slot, 0:kn * 128, :], (((1,), (1,)), ((), ())), preferred_element_type=F32)

    lane_c = lax.broadcasted_iota(jnp.int32, (CHUNK, 128), 1)

    def pick_z(t, row, zs):
        rs = slice(row, row + CHUNK)
        rel, az = rel_ref[rs, :], az_ref[rs, :]
        for k, z in enumerate(zs):
            az = jnp.where(rel == t * TILE + k * 128, z, az)
        az_ref[rs, :] = az

    def epilogue(t, zref, part, pick=True):
        last = isinstance(t, int) and t == n_tiles - 1
        kn = last_k if last else TILE // 128
        for row in range(part.start, part.stop, CHUNK):
            rs = slice(row, row + CHUNK)
            zs = [zref[rs, k * 128:(k + 1) * 128] for k in range(kn)]
            if last:
                zs[-1] = jnp.where(lane_c < last_lanes, zs[-1], -jnp.inf)
            c = c_ref[rs, :]
            m2 = functools.reduce(jnp.maximum, zs) * c
            es = [jnp.exp2(z * c - m2) for z in zs]
            st = functools.reduce(jnp.add, es)
            mo = m_ref[rs, :]
            mn = jnp.maximum(mo, m2)
            s_ref[rs, :] = s_ref[rs, :] * jnp.exp2(mo - mn) + st * jnp.exp2(m2 - mn)
            m_ref[rs, :] = mn
            if row < n_seq:
                continue
            rs = slice(row - n_seq, row - n_seq + CHUNK)
            mt_ref[t, rs, :] = m2
            for k in range(kn):
                wd = 128 if not (last and k == kn - 1) else last_lanes
                cs = pl.ds(t * TILE + k * 128, wd)
                if not isinstance(t, int):
                    cs = pl.ds(pl.multiple_of(t * TILE + k * 128, 128), wd)
                ex_ref[rs, cs] = es[k] if wd == 128 else es[k][:, :wd]
            if pick:
                pick_z(t, row - n_seq, zs)

    zbuf = (za, zb)
    whole = slice(0, n_all)
    half1 = slice(0, n_seq + rows // 2)
    half2 = slice(n_seq + rows // 2, n_all)

    def step(ts, prev):
        for t, zref in ts:
            dot(t, zref, whole)
            epilogue(*prev, whole)
            prev = (t, zref)

    small[0].wait()
    small[1].wait()
    w_copy(0).wait()
    dot(0, za, half1)
    norm_some(list(range(draft)), half_seq, [half_seq] * draft)
    reorder(half_seq, half_seq)
    t_row = t_ref[...]
    d_f = dt_ref[...].astype(F32)
    base = me * vocab
    lane_s = lax.broadcasted_iota(jnp.int32, (draft, n_seq), 1)
    t_all = jnp.broadcast_to(LOG2E / t_row, (draft, n_seq))
    for b in range(n_seq):
        pick = lane_s == b
        r8 = slice(b * draft, (b + 1) * draft)
        c = jnp.sum(jnp.where(pick, t_all, 0.0), axis=1, keepdims=True)
        d = jnp.sum(jnp.where(pick, d_f, 0.0), axis=1, keepdims=True)
        c_ref[n_seq + b * draft:n_seq + (b + 1) * draft, :] = jnp.broadcast_to(c, (draft, 128))
        loc = jnp.broadcast_to(d, (draft, 128)).astype(jnp.int32) - base
        owned = (loc >= 0) & (loc < vocab)
        rel_ref[r8, :] = jnp.where(owned, loc - lane8, -vocab)
    diag = lax.broadcasted_iota(jnp.int32, (n_seq, n_seq), 0) == lax.broadcasted_iota(jnp.int32, (n_seq, n_seq), 1)
    cb = jnp.sum(jnp.where(diag, jnp.broadcast_to(LOG2E / t_row, (n_seq, n_seq)), 0.0), axis=1, keepdims=True)
    c_ref[0:n_seq, :] = jnp.broadcast_to(cb, (n_seq, 128))

    dot(0, za, half2)
    w_copy(SLOTS - 2).start()
    w_copy(SLOTS - 1).start()
    for t in range(6):
        q_copy(t).start()
    w_copy(1).wait()
    w_copy(2).wait()
    step([(1, zb), (2, za)], (0, za))
    first = n_tiles - HALVED
    n_body = (first - 3) // BODY

    def body(i, carry):
        t = BODY * i + 3
        for u in range(BODY):
            w_copy(t + u).wait()

        @pl.when(i == 0)
        def _():
            for u in range(SLOTS, SLOTS + 3):
                w_copy(u).start()
            for u in range(6, 10):
                q_copy(u).start()

        @pl.when(i == 1)
        def _():
            for u in range(SLOTS + 3, n_tiles):
                w_copy(u).start()
            for u in range(10, n_tiles):
                q_copy(u).start()

        step([(t + u, zbuf[(u + 1) % 2]) for u in range(BODY)], (t - 1, za))
        return carry

    lax.fori_loop(0, n_body, body, 0)
    for t in range(first, n_tiles):
        w_copy(t).wait()
    prev = (first - 1, za, whole)
    u = 1
    for t in range(first, n_tiles):
        dot(t, zbuf[u], half1)
        epilogue(*prev)
        prev = (t, zbuf[u], half1)
        u = 1 - u

    def exchange(src, dst, ssem, rsem):
        out = []
        for k, p in enumerate(peers):
            cp = pltpu.make_async_remote_copy(
                src_ref=src, dst_ref=dst.at[me], send_sem=ssem.at[k], recv_sem=rsem.at[me],
                device_id={"tp": p}, device_id_type=MESH)
            cp.start()
            out.append(cp)
        return out

    def finish(src, dst, rsem):
        for p in peers:
            pltpu.make_async_remote_copy(
                src_ref=src, dst_ref=dst.at[p], send_sem=rsem.at[p], recv_sem=rsem.at[p],
                device_id={"tp": p}, device_id_type=MESH).wait_recv()

    def drain(cps):
        for cp in cps:
            cp.wait_send()

    def spread(row):
        return jnp.transpose(jnp.broadcast_to(row, (128, 128)))

    def log_sum(start):
        blk = slice(start, start + 128)
        mt = jnp.transpose(m_ref[blk, :])
        st = jnp.transpose(s_ref[blk, :])
        mrow = jnp.max(mt, axis=0, keepdims=True)
        return mrow + jnp.log(jnp.sum(st * jnp.exp2(mt - mrow), axis=0, keepdims=True)) * LOG2E

    def log_total(recv):
        parts = [recv[i] for i in range(n_dev)]
        mx = functools.reduce(jnp.maximum, parts)
        return mx + jnp.log(functools.reduce(jnp.add, [jnp.exp2(v - mx) for v in parts])) * LOG2E

    hb = n_blk // 2

    def first_half():
        for i in range(hb):
            send1[i:i + 1, :] = log_sum(n_seq + i * 128)
        send1[hb:hb + 1, :] = log_sum(0)
        pl.semaphore_wait(barrier, n_dev - 1)
        cps1 = exchange(send1, recv1, ssem1, rsem1)
        recv1[me] = send1[...]
        return cps1

    for t in range(first, n_tiles):
        dot(t, zbuf[u], half2)
        epilogue(*prev)
        prev = (t, zbuf[u], half2)
        u = 1 - u
        if t == n_tiles - 4:
            cps1 = first_half()
    if HALVED < 4:
        cps1 = first_half()
    epilogue(*prev, pick=False)
    for i in range(hb, n_blk):
        send2[i - hb:i - hb + 1, :] = log_sum(n_seq + i * 128)
    cps2 = exchange(send2, recv2, ssem2, rsem2)
    recv2[me] = send2[...]

    for row in range(half2.start, half2.stop, CHUNK):
        rs = slice(row, row + CHUNK)
        pick_z(n_tiles - 1, row - n_seq, [prev[1][rs, k * 128:(k + 1) * 128] for k in range(last_k)])
    for t in range(n_tiles):
        q_copy(t).wait()

    def pick_q(i, carry):
        rs = pl.ds(pl.multiple_of(i * 16, 16), 16)
        rel = rel_ref[rs, :]
        aqs = [jnp.full((16, 128), -1.0, F32) for _ in range(4)]
        for v in range(n_full):
            aqs[v % 4] = jnp.where(rel == v * 128, q_scr[rs, v * 128:(v + 1) * 128], aqs[v % 4])
        if tail:
            qv = jnp.concatenate(
                [q_scr[rs, n_full * 128:vocab], jnp.zeros((16, 128 - tail), F32)], axis=1)
            aqs[0] = jnp.where(rel == n_full * 128, qv, aqs[0])
        aq_ref[rs, :] = functools.reduce(jnp.maximum, aqs)
        return carry

    lax.fori_loop(0, rows // 16, pick_q, 0)
    s_tok, q_tok = [], []
    for i in range(n_blk):
        blk = slice(i * 128, (i + 1) * 128)
        s_tok.append(jnp.max(jnp.transpose(az_ref[blk, :] * c_ref[n_seq + i * 128:n_seq + (i + 1) * 128, :]), axis=0, keepdims=True))
        q_tok.append(jnp.max(jnp.transpose(aq_ref[blk, :]), axis=0, keepdims=True))
    s_tok = jnp.concatenate(s_tok, axis=0)
    q_tok = jnp.concatenate(q_tok, axis=0)

    def excess(i, carry):
        n = 8 * UNROLL
        rs = pl.ds(pl.multiple_of(i * n, n), n)
        rz = pl.ds(pl.multiple_of(i * n + n_seq, 8), n)
        lb = m_ref[rz, :]
        accs = [jnp.zeros((n, 128), F32) for _ in range(2)]
        for t in range(n_tiles):
            coef = jnp.exp2(mt_ref[t, rs, :] - lb)
            for k in range(TILE // 128):
                v = t * (TILE // 128) + k
                if v < n_full:
                    cs = slice(v * 128, (v + 1) * 128)
                    d = jnp.maximum(ex_ref[rs, cs] * coef - q_scr[rs, cs], 0.0)
                    ex_ref[rs, cs] = d
                    accs[k % 2] = accs[k % 2] + d
                elif v == n_full and tail:
                    cs = slice(v * 128, v * 128 + tail)
                    d = jnp.maximum(ex_ref[rs, cs] * coef[:, :tail] - q_scr[rs, cs], 0.0)
                    ex_ref[rs, cs] = d
                    accs[k % 2] = accs[k % 2] + jnp.concatenate([d, jnp.zeros((n, 128 - tail), F32)], axis=1)
        s_ref[rz, :] = accs[0] + accs[1]
        return carry

    per_half = rows // (16 * UNROLL)

    def norm_part(i):
        blk = slice(n_seq + i * 128, n_seq + (i + 1) * 128)
        return jnp.sum(jnp.transpose(s_ref[blk, :]), axis=0, keepdims=True)

    finish(send1, recv1, rsem1)
    lse_a = log_total(recv1)
    for i in range(hb):
        m_ref[n_seq + i * 128:n_seq + (i + 1) * 128, :] = spread(lse_a[i:i + 1, :])
    lax.fori_loop(0, per_half, excess, 0)
    for i in range(hb):
        send3[i:i + 1, :] = norm_part(i)
    cps3 = exchange(send3, recv3, ssem3, rsem3)
    recv3[me] = send3[...]

    finish(send2, recv2, rsem2)
    lse_b = log_total(recv2)
    for i in range(hb, n_blk):
        m_ref[n_seq + i * 128:n_seq + (i + 1) * 128, :] = spread(lse_b[i - hb:i - hb + 1, :])
    lax.fori_loop(per_half, 2 * per_half, excess, 0)
    for i in range(hb, n_blk):
        send4[i - hb:i - hb + 1, :] = norm_part(i)
    lse = jnp.concatenate([lse_a[0:hb], lse_b[0:n_blk - hb]], axis=0)
    acc = jnp.where(q_tok >= 0.0, jnp.minimum(1.0, jnp.exp2(s_tok - lse) / q_tok), 0.0)
    send4[n_blk - hb:2 * n_blk - hb, :] = acc
    cps4 = exchange(send4, recv4, ssem4, rsem4)
    recv4[me] = send4[...]
    st_ref[2 * n_blk:2 * n_blk + 1, :] = lse_a[hb:hb + 1, :] * LN2

    drain(cps1 + cps2 + cps3)
    finish(send3, recv3, rsem3)
    st_ref[0:hb, :] = functools.reduce(jnp.add, [recv3[i] for i in range(n_dev)])
    finish(send4, recv4, rsem4)
    st_ref[hb:2 * n_blk, :] = functools.reduce(jnp.add, [recv4[i] for i in range(n_dev)])
    drain(cps4)


def _scale_kernel(n_seq, draft, vocab, ex_ref, st_ref,
                  acc_hbm, norm_hbm, res_hbm, lse_hbm, acc_ref, norm_ref, lse_ref, nb_ref, ab_ref, buf, sem, osem):
    rows = n_seq * draft
    step = buf.shape[1]
    n = rows // step
    slots = buf.shape[0]
    lane8 = lax.broadcasted_iota(jnp.int32, (8, 128), 1)

    def copy(i):
        slot = lax.rem(i, slots) if not isinstance(i, int) else i % slots
        return pltpu.make_async_copy(
            buf.at[slot], res_hbm.at[pl.ds(pl.multiple_of(i * step, step), step), :], sem.at[slot])

    n_full = vocab // 128
    tail = vocab - n_full * 128

    def body(i, carry):
        slot = lax.rem(i, slots)

        @pl.when(i >= slots)
        def _():
            copy(i - slots).wait()

        for r in range(step // 8):
            rs = pl.ds(pl.multiple_of(i * step + r * 8, 8), 8)
            inv = 1.0 / nb_ref[rs, :]
            for v in range(n_full):
                cs = slice(v * 128, (v + 1) * 128)
                buf[slot, r * 8:r * 8 + 8, cs] = ex_ref[rs, cs] * inv
            if tail:
                cs = slice(n_full * 128, vocab)
                buf[slot, r * 8:r * 8 + 8, cs] = ex_ref[rs, cs] * inv[:, :tail]
        copy(i).start()
        return carry

    n_blk = rows // 128

    def spread(dst, row):
        for i in range(n_blk):
            dst[i * 128:(i + 1) * 128, :] = jnp.transpose(
                jnp.broadcast_to(st_ref[row + i:row + i + 1, :], (128, 128)))

    def by_seq(src):
        out = jnp.zeros((8, 128), F32)
        for b in range(n_seq):
            out = jnp.where(lane8 == b, src[b * draft:(b + 1) * draft, :], out)
        return out[0:draft, 0:n_seq]

    spread(nb_ref, 0)
    lax.fori_loop(0, slots, body, 0)
    spread(ab_ref, n_blk)
    acc_ref[...] = by_seq(ab_ref)
    norm_ref[...] = by_seq(nb_ref)
    lse_ref[...] = st_ref[2 * n_blk:2 * n_blk + 1, 0:n_seq]
    outs = [pltpu.make_async_copy(src, dst, osem.at[i]) for i, (src, dst) in enumerate(
        ((acc_ref, acc_hbm), (norm_ref, norm_hbm), (lse_ref, lse_hbm)))]
    for cp in outs:
        cp.start()
    lax.fori_loop(slots, n, body, 0)
    for cp in outs:
        cp.wait()
    for s in range(slots):
        copy(n - slots + s).wait()


def solution(mesh):
    n_dev = mesh.shape["tp"]

    def local_step(hidden, norm_gain, w_head, draft_probs, draft_tokens, value_a11):
        n_seq, n_pos, d_model = hidden.shape
        draft = n_pos - 1
        vocab = w_head.shape[1]
        rows = n_seq * draft
        n_all = rows + n_seq
        n_tiles = pl.cdiv(vocab, TILE)
        h = jnp.transpose(hidden, (1, 0, 2))
        w = jnp.transpose(w_head)
        q = draft_probs.reshape(rows, vocab)
        vm = pl.BlockSpec(memory_space=pltpu.VMEM)
        anyspec = pl.BlockSpec(memory_space=pl.ANY)
        dma = pltpu.SemaphoreType.DMA
        stat = pltpu.VMEM((n_all, 128), F32)
        n_blk = rows // 128
        msgs = (n_blk // 2 + 1, n_blk - n_blk // 2, n_blk // 2, 2 * n_blk - n_blk // 2)
        ex, st = pl.pallas_call(
            functools.partial(_main_kernel, n_dev, n_seq, draft, d_model, vocab),
            out_shape=(
                pltpu.VMEM((rows, vocab), F32),
                pltpu.VMEM((2 * n_blk + 8, 128), F32),
            ),
            in_specs=[anyspec] * 6,
            out_specs=(vm, vm),
            scratch_shapes=[
                pltpu.VMEM((1, d_model), F32),
                pltpu.VMEM((draft, n_seq), jnp.int32),
                pltpu.VMEM((1, n_seq), F32),
                pltpu.VMEM((n_all, d_model), BF16),
                pltpu.VMEM((SLOTS, TILE, d_model), BF16),
                pltpu.VMEM((rows, vocab), F32),
                pltpu.VMEM((n_all, TILE), F32),
                pltpu.VMEM((n_all, TILE), F32),
                pltpu.VMEM((n_all, 128), F32),
                pltpu.VMEM((rows, 128), jnp.int32),
                stat, stat,
                pltpu.VMEM((rows, 128), F32),
                pltpu.VMEM((rows, 128), F32),
                pltpu.VMEM((n_tiles, rows + 8, 128), F32),
                *[pltpu.VMEM((m, 128), F32) for m in msgs],
                *[pltpu.VMEM((n_dev, m, 128), F32) for m in msgs],
                dma((3,)), dma((n_pos,)), dma((SLOTS,)), dma((n_tiles,)),
                *[dma((n_dev,)) for _ in range(8)],
            ],
            compiler_params=pltpu.CompilerParams(
                collective_id=0, has_side_effects=True, vmem_limit_bytes=48 * 2**20),
        )(norm_gain.reshape(1, d_model), jnp.transpose(draft_tokens), value_a11.reshape(1, n_seq), h, w, q)

        vmc = lambda a: pltpu.with_memory_space_constraint(a, pltpu.VMEM)
        acc, norm, res, lse = pl.pallas_call(
            functools.partial(_scale_kernel, n_seq, draft, vocab),
            out_shape=(
                jax.ShapeDtypeStruct((draft, n_seq), F32),
                jax.ShapeDtypeStruct((draft, n_seq), F32),
                jax.ShapeDtypeStruct((rows, vocab), F32),
                jax.ShapeDtypeStruct((1, n_seq), F32),
            ),
            in_specs=[vm, vm],
            out_specs=(anyspec,) * 4,
            scratch_shapes=[
                pltpu.VMEM((draft, n_seq), F32), pltpu.VMEM((draft, n_seq), F32), pltpu.VMEM((1, n_seq), F32),
                pltpu.VMEM((rows, 128), F32), pltpu.VMEM((rows, 128), F32),
                pltpu.VMEM((8, 16, vocab), F32), dma((8,)), dma((3,)),
            ],
            compiler_params=pltpu.CompilerParams(vmem_limit_bytes=16 * 2**20),
        )(vmc(ex), vmc(st))
        return (jnp.transpose(acc), jnp.transpose(norm), res.reshape(n_seq, draft, vocab), lse.reshape(n_seq))

    return jax.shard_map(
        local_step,
        mesh=mesh,
        in_specs=(P('dp', None, None), P(), P(None, 'tp'), P('dp', None, 'tp'), P('dp', None), P('dp')),
        out_specs=(P('dp', None), P('dp', None), P('dp', None, 'tp'), P('dp')),
        check_vma=False,
    )
```
